1024 devices in a mesh: theta: 64 (over x_hi, z, core), band: 16 (over y, x_lo).
Axes of the slice: x: 8 (x_hi: 4, x_lo: 2; x = x_hi * 2 + x_lo), y: 8, z: 8, core: 2. Of those that a mesh axis runs over, the one named last changes fastest.
Arguments:
- basis: float32 [4, 5, 16, 8192], P(None, None, 'band', 'theta'), may hold values from -8 to 8
- jac_block: float32 [5, 5, 16, 8192], P(None, None, 'band', 'theta'), may hold values from -3 to 3
- face_coef: float32 [4, 5, 16, 8192], P(None, None, 'band', 'theta'), may hold values from 0.1 to 1.1
- panel_inverse: bfloat16 [16, 128, 320, 640], P('band', 'theta'), may hold values from -0.2 to 1.2
- rotor_offset: int32 [1], replicated, may hold values from 4032 to 4159
Outputs:
- precond: float32 [5, 16, 8192], P(None, 'band', 'theta')
- v_next: float32 [5, 16, 8192], P(None, 'band', 'theta')
- hess: float32 [5], replicated
The draws below stay inside these ranges and needn't reach their ends.
All inputs are finite; a program needn't handle non-finite values.
Results may differ from the reference program's by a relative error of at most 0.0029.
Values may be sent and summed in bfloat16 or wider, within the bound.
A program may use at most 32 MiB of HBM per device.

```python
import jax
import jax.numpy as jnp
from jax import lax

NCOMP = 5
PANEL = 128
KB = 4
HALF = 64
NB = 16
NT = 8192
NPAN = 128
PROWS = 320
PCOLS = 640
IFACE = 8
NU = 655360
N_THETA = 64


def draw_basis(key, part):
    first, second = jax.random.split(jax.random.fold_in(key, 11))
    own = jax.random.normal(first, (KB, NCOMP, NB, NT), jnp.float32)
    shared = jax.random.normal(second, (1, NCOMP, NB, NT), jnp.float32)
    return jnp.clip(0.6 * own + 0.8 * shared, -8.0, 8.0)


def draw_panel_inverse(key, part):
    noise = jax.random.normal(jax.random.fold_in(key, 23), (NB, NPAN, PROWS, PCOLS), jnp.float32)
    noise = jnp.clip(noise * (0.6 / PCOLS ** 0.5), -0.19, 0.19)
    rows = jnp.arange(PROWS, dtype=jnp.int32)
    side = jnp.arange(NPAN, dtype=jnp.int32) % 2
    column = (rows // HALF)[None, :] * PANEL + (rows % HALF)[None, :] + HALF * (1 - side)[:, None]
    target = (jnp.arange(PCOLS, dtype=jnp.int32)[None, None, :] == column[:, :, None]).astype(jnp.float32)
    return (noise + target[None]).astype(jnp.bfloat16)


def block_levels(rng, shape, pieces, smallest, high):
    level, own = 1.0, jax.random.fold_in(rng, 6)
    for axis_at, parts in pieces:
        steps = jnp.exp(jax.random.uniform(jax.random.fold_in(own, axis_at), (parts,), jnp.float32, smallest / len(pieces), high / len(pieces)))
        level = level * jnp.repeat(steps, shape[axis_at] // parts).reshape([-1 if axis == axis_at else 1 for axis in range(len(shape))])
    return level


def centred(key, shape, deviation, most, pieces=(), kind=jnp.bfloat16):
    drawn = jax.random.normal(key, shape, jnp.float32) * deviation
    if len(pieces) > 0:
        drawn = block_levels(key, shape, pieces, -0.22, 0.18) * drawn
    return jnp.clip(drawn, min=-most, max=most).astype(kind)


def setup_inputs(seed: int = 0) -> dict:
    splits = jax.random.split(jax.random.key(seed), 6)
    basis = draw_basis(jax.random.fold_in(splits[5], 71), 0)
    jac_block = centred(splits[1], (NCOMP, NCOMP, NB, NT), 0.5, 3.0, ((2, 16), (3, 64)), jnp.float32)
    face_coef = jnp.clip(0.1 + 1 * jax.random.uniform(splits[2], (4, NCOMP, NB, NT), jnp.float32) ** block_levels(splits[2], (4, NCOMP, NB, NT), ((2, 16), (3, 64)), -0.2, 0.2), 0.1, 1.1)
    panel_inverse = draw_panel_inverse(jax.random.fold_in(splits[5], 71), 0)
    rotor_offset = jax.random.randint(splits[4], (1,), NT // 2 - HALF, NT // 2 + HALF).astype(jnp.int32)
    return dict(basis=basis, jac_block=jac_block, face_coef=face_coef, panel_inverse=panel_inverse, rotor_offset=rotor_offset)


def reference(basis, jac_block, face_coef, panel_inverse, rotor_offset):
    current = basis[KB - 1]
    resid16 = current.astype(jnp.bfloat16)
    starts = jnp.arange(N_THETA, dtype=jnp.int32)[:, None] * PANEL - HALF
    window = (starts + jnp.arange(2 * PANEL, dtype=jnp.int32)[None, :]) % NT
    extended = resid16[:, :, window]
    panels = extended.reshape(NCOMP, NB, N_THETA, 2, PANEL).transpose(1, 2, 3, 0, 4).reshape(NB, NPAN, PCOLS)

    def one_row(pair):
        inverse_row, panel_row = pair
        return jnp.einsum('pij,pj->pi', inverse_row.astype(jnp.float32), panel_row.astype(jnp.float32))
    owned = lax.map(one_row, (panel_inverse, panels))
    precond = owned.reshape(NB, N_THETA, 2, NCOMP, HALF).transpose(3, 0, 1, 2, 4).reshape(NCOMP, NB, NT)
    offset = rotor_offset[0]
    cells = jnp.arange(NT, dtype=jnp.int32)
    theta_minus = jnp.roll(precond, 1, axis=2)
    theta_plus = jnp.roll(precond, -1, axis=2)
    zero_row = jnp.zeros((NCOMP, 1, NT), jnp.float32)
    band_minus = jnp.concatenate([zero_row, precond[:, :-1]], axis=1)
    band_plus = jnp.concatenate([precond[:, 1:], zero_row], axis=1)
    low_shift = precond[:, IFACE - 1][:, (cells - offset + NT) % NT]
    up_shift = precond[:, IFACE][:, (cells + offset) % NT]
    band_minus = band_minus.at[:, IFACE].set(low_shift)
    band_plus = band_plus.at[:, IFACE - 1].set(up_shift)
    image = 6.0 * precond + lax.optimization_barrier(jnp.sum(jac_block * precond[None], axis=1))
    image = image - (face_coef[0] * theta_minus + face_coef[1] * theta_plus + face_coef[2] * band_minus + face_coef[3] * band_plus)
    proj = lax.optimization_barrier(jnp.sum(basis * image[None], axis=(1, 2, 3))) / NU
    ortho = image - lax.optimization_barrier(jnp.sum(proj[:, None, None, None] * basis, axis=0))
    hnorm = jnp.sqrt(jnp.sum(ortho * ortho) / NU + 1e-06)
    v_next = ortho / hnorm
    hess = jnp.concatenate([proj, hnorm[None]])
    return (precond, v_next, hess)
```

```python
import functools
import itertools

import jax
import jax.numpy as jnp
from jax import lax
from jax.experimental import pallas as pl
from jax.experimental.pallas import tpu as pltpu
from jax.sharding import Mesh
from jax.sharding import PartitionSpec as P

THETA = ("theta_0", "theta_1", "theta_2")
BAND = ("band_0", "band_1")
NAMES = ("theta_0", "theta_1", "theta_2", "band_0", "band_1")
MESH = pl.DeviceIdType.MESH

SIZES = {"x": 8, "y": 8, "z": 8, "c": 2}
PHASES = (("x",), ("y",), ("z", "c"))
F32 = jnp.float32
KB, NC, W = 4, 5, 128
PAIRS = [(a, b) for a in range(KB) for b in range(a, KB)]
IMG = KB + len(PAIRS)


def ring_distance(d, n):
    return min(d, n - d)


def offsets_of(axes):
    every = itertools.product(*[range(SIZES[a]) for a in axes])
    some = [o for o in every if any(o)]
    return sorted(
        some, key=lambda o: -sum(ring_distance(d, SIZES[a]) for d, a in zip(o, axes))
    )


def add_mod(v, d, n):
    if d == 0:
        return v
    s = v + d
    return jnp.where(s >= n, s - n, s)


def moved(here, axes, offset):
    t0, z, c, y, xl = here
    for a, d in zip(axes, offset):
        if d == 0:
            continue
        if a == "x":
            if d % 2:
                s = t0 + xl + d // 2
                t0 = jnp.where(s >= 4, s - 4, s)
                xl = 1 - xl
            else:
                t0 = add_mod(t0, d // 2, 4)
        elif a == "y":
            y = add_mod(y, d, 8)
        elif a == "z":
            z = add_mod(z, d, 8)
        else:
            c = 1 - c
    return (t0, z, c, y, xl)


def theta_next(here):
    t0, z, c, y, xl = here
    z1 = z + c
    over = z1 >= 8
    t1 = jnp.where(over, t0 + 1, t0)
    return (jnp.where(t1 >= 4, t1 - 4, t1), jnp.where(over, 0, z1), 1 - c, y, xl)


def theta_prev(here):
    t0, z, c, y, xl = here
    z1 = z - 1 + c
    under = z1 < 0
    t1 = jnp.where(under, t0 - 1, t0)
    return (jnp.where(t1 < 0, t1 + 4, t1), jnp.where(under, 7, z1), 1 - c, y, xl)


def band_next(here):
    t0, z, c, y, xl = here
    y1 = y + xl
    return (t0, z, c, jnp.where(y1 >= 8, y1 - 8, y1), 1 - xl)


def band_prev(here):
    t0, z, c, y, xl = here
    y1 = y - 1 + xl
    return (t0, z, c, jnp.where(y1 < 0, y1 + 8, y1), 1 - xl)


def across(here):
    t0, z, c, y, xl = here
    return (add_mod(t0, 2, 4), z, c, 7 - y, 1 - xl)


def kernel(
    total,
    basis_hbm,
    jac_hbm,
    face_hbm,
    pinv_hbm,
    off_hbm,
    precond_out,
    v_out,
    hess_out,
    basis,
    jac,
    face,
    pinv,
    off,
    mine,
    halo,
    bown,
    bhalo,
    prec,
    near,
    rotor,
    image_buf,
    load_sems,
    halo_send,
    halo_recv,
    near_send,
    near_recv,
    rotor_send,
    rotor_recv,
    *phase_refs,
):
    here = tuple(lax.axis_index(n) for n in NAMES)
    t0, z, c, y, xl = here
    band = y * 2 + xl
    at_edge = (band == 7) | (band == 8)
    left, right = theta_prev(here), theta_next(here)
    below, above = band_prev(here), band_next(here)
    opposite = across(here)
    opposite3 = (theta_prev(opposite), opposite, theta_next(opposite))

    loads = []
    zero3 = jnp.zeros((3, W), F32)
    for i in range(KB):
        loads.append((basis_hbm.at[i, :, 0, :], basis.at[i, pl.ds(0, NC), :], 0 if i == KB - 1 else 1))
    for w in range(NC):
        loads.append((jac_hbm.at[:, w, 0, :], jac.at[w, pl.ds(0, NC), :], 1))
    for d in range(4):
        loads.append((face_hbm.at[d, :, 0, :], face.at[d, pl.ds(0, NC), :], 1))
    copies = [
        pltpu.make_async_copy(src, dst, load_sems.at[k]) for k, (src, dst, _) in enumerate(loads)
    ]
    copies[KB - 1].start()
    pinv_copy = pltpu.make_async_copy(pinv_hbm.at[0], pinv, load_sems.at[len(loads)])
    pinv_copy.start()
    off_copy = pltpu.make_async_copy(off_hbm, off, load_sems.at[len(loads) + 1])
    off_copy.start()
    for k, copy in enumerate(copies):
        if k != KB - 1:
            copy.start()

    barrier = pltpu.get_barrier_semaphore()
    partners = [left, right, below, above]
    for axes in PHASES:
        partners += [moved(here, axes, o) for o in offsets_of(axes)]
    for p in partners:
        pl.semaphore_signal(barrier, inc=1, device_id=p, device_id_type=MESH)

    @pl.when(at_edge)
    def _():
        for p in opposite3:
            pl.semaphore_signal(barrier, inc=1, device_id=p, device_id_type=MESH)

    for i in range(KB):
        basis[i, NC:, :] = zero3
    for w in range(NC):
        jac[w, NC:, :] = zero3
    for d in range(4):
        face[d, NC:, :] = zero3

    lane = lax.broadcasted_iota(jnp.int32, (8, W), 1)
    row = lax.broadcasted_iota(jnp.int32, (8, W), 0)

    copies[KB - 1].wait()
    own = pltpu.roll(basis[KB - 1].astype(jnp.bfloat16).astype(F32), W // 2, 1)
    mine[...] = own

    pl.semaphore_wait(barrier, len(partners) + jnp.where(at_edge, 3, 0))
    halo_copies = []
    for k, p in enumerate((left, right)):
        copy = pltpu.make_async_remote_copy(
            mine, halo.at[1 - k], halo_send.at[k], halo_recv.at[1 - k],
            device_id=p, device_id_type=MESH,
        )
        copy.start()
        halo_copies.append(copy)

    pinv_copy.wait()
    cols = lax.broadcasted_iota(jnp.int32, (320, 640), 1) % W
    a0, a1 = pinv[0], pinv[1]
    bown[...] = jnp.where(cols < W // 2, a1, a0)
    bhalo[...] = jnp.where(cols < W // 2, a0, a1)
    xrow = lax.broadcasted_iota(jnp.int32, (W, W), 0)
    xlane = lax.broadcasted_iota(jnp.int32, (W, W), 1)
    same = (xrow < W // 2) == (xlane < W // 2)

    def spread(vec, keep):
        parts = [
            jnp.where(keep, jnp.broadcast_to(vec[u : u + 1, :], (W, W)), 0.0).astype(jnp.bfloat16)
            for u in range(NC)
        ]
        return jnp.concatenate(parts, axis=1)

    def times(mat, rhs):
        return lax.dot_general(
            mat, rhs, (((1,), (1,)), ((), ())), preferred_element_type=F32
        )

    r_own = times(bown[...], spread(own, jnp.logical_not(same)))
    pick = lax.broadcasted_iota(jnp.int32, (64, W), 0) == lax.broadcasted_iota(
        jnp.int32, (64, W), 1
    ) % 64

    def fold(r):
        return [
            jnp.sum(jnp.where(pick, r[u * 64 : (u + 1) * 64, :], 0.0), axis=0, keepdims=True)
            for u in range(NC)
        ]

    own_part = fold(r_own)

    for k, copy in enumerate(copies):
        if k != KB - 1:
            copy.wait()
    off_copy.wait()

    gram_rows = [jnp.sum(basis[a] * basis[b], axis=0, keepdims=True) for a, b in PAIRS]
    gram_rows += [jnp.zeros((1, W), F32)] * (16 - len(PAIRS))
    gram_sum = jnp.sum(jnp.concatenate(gram_rows, axis=0), axis=1, keepdims=True)
    lane16 = lax.broadcasted_iota(jnp.int32, (16, W), 1)
    row16 = lax.broadcasted_iota(jnp.int32, (16, W), 0)
    gram_line = jnp.sum(jnp.where(lane16 == row16 + KB, gram_sum, 0.0), axis=0, keepdims=True)
    gram_line = jnp.where(lane16[:1] < IMG, gram_line, 0.0)

    for k, copy in enumerate(halo_copies):
        copy.wait_recv()
    ph = jnp.where(lane < W // 2, halo[0], halo[1])
    halo_part = fold(times(bhalo[...], spread(ph, same)))
    zero1 = jnp.zeros((1, W), F32)
    pre = jnp.concatenate([a + b for a, b in zip(own_part, halo_part)] + [zero1] * 3, axis=0)
    prec[...] = pre

    near_copies = []
    for slot, p in ((3, below), (2, above), (1, left), (0, right)):
        copy = pltpu.make_async_remote_copy(
            prec, near.at[slot], near_send.at[slot], near_recv.at[slot],
            device_id=p, device_id_type=MESH,
        )
        near_copies.append(copy)
    rotor_copies = []
    for k in range(3):
        rotor_copies.append(
            pltpu.make_async_remote_copy(
                prec, rotor.at[2 - k], rotor_send.at[k], rotor_recv.at[2 - k],
                device_id=opposite3[k], device_id_type=MESH,
            )
        )

    @pl.when(at_edge)
    def _():
        for copy in rotor_copies:
            copy.start()

    for copy in near_copies:
        copy.start()

    base = 6.0 * pre
    for w in range(NC):
        base = base + jac[w] * pre[w : w + 1, :]

    for copy in near_copies:
        copy.wait_recv()
    tm = pltpu.roll(jnp.where(lane == W - 1, near[0], pre), 1, 1)
    tp = pltpu.roll(jnp.where(lane == 0, near[1], pre), W - 1, 1)
    base = base - face[0] * tm - face[1] * tp
    image_buf[...] = base
    near[2] = jnp.where(band == 0, 0.0, near[2])
    near[3] = jnp.where(band == 15, 0.0, near[3])

    @pl.when(at_edge)
    def _():
        for copy in rotor_copies:
            copy.wait_recv()
        shift = off[0] - 4032
        o = jnp.where(band == 7, shift, W - shift)
        joined = jnp.where(
            lane >= 64 + o, rotor[0], jnp.where(lane < o - 64, rotor[2], rotor[1])
        )
        turn = 64 - o
        turn = jnp.where(turn < 0, turn + W, turn)
        crossed = pltpu.roll(joined, turn, 1)
        near[2] = jnp.where(band == 8, crossed, near[2])
        near[3] = jnp.where(band == 7, crossed, near[3])

    image = image_buf[...] - face[2] * near[2] - face[3] * near[3]
    image_buf[...] = image

    late = [jnp.sum(basis[i] * image, axis=0, keepdims=True) for i in range(KB)]
    late.append(jnp.sum(image * image, axis=0, keepdims=True))
    late += [zero1] * 3
    late_sum = jnp.sum(jnp.concatenate(late, axis=0), axis=1, keepdims=True)
    want = jnp.where(row < KB, row, IMG)
    want = jnp.where(row > KB, -1, want)
    line = gram_line + jnp.sum(jnp.where(lane == want, late_sum, 0.0), axis=0, keepdims=True)

    ends = []
    for k, axes in enumerate(PHASES):
        src, slots, ssem, rsem = phase_refs[4 * k : 4 * k + 4]
        some = offsets_of(axes)
        n = len(some)
        src[...] = line
        for s, o in enumerate(some):
            pltpu.make_async_remote_copy(
                src, slots.at[pl.ds(s, 1), :], ssem, rsem,
                device_id=moved(here, axes, o), device_id_type=MESH,
            ).start()
        everything = slots.at[pl.ds(0, n), :]
        whole = pltpu.make_async_remote_copy(
            everything, everything, ssem, rsem, device_id=right, device_id_type=MESH
        )
        whole.wait_recv()
        ends.append(whole)
        line = line + jnp.sum(slots[pl.ds(0, n), :], axis=0, keepdims=True)

    line = line * (1.0 / total)
    spread16 = jnp.sum(jnp.where(lane16 == row16, line, 0.0), axis=1, keepdims=True)
    at = [jnp.broadcast_to(spread16[i : i + 1, :], (1, W)) for i in range(IMG + 1)]
    proj = at[:KB]
    gram = {pair: at[KB + k] for k, pair in enumerate(PAIRS)}
    squares = at[IMG]
    ortho = image
    for i in range(KB):
        squares = squares - 2.0 * proj[i] * proj[i]
        ortho = ortho - proj[i] * basis[i]
    for (a, b), g in gram.items():
        term = proj[a] * g * proj[b]
        squares = squares + (term if a == b else 2.0 * term)
    hnorm = jnp.sqrt(squares + 1e-06)
    v = ortho / hnorm
    for u in range(NC):
        precond_out[u] = prec[u : u + 1, :]
        v_out[u] = v[u : u + 1, :]
    hess_out[...] = jnp.where(lane[:1] < KB, line, hnorm)

    for copy in halo_copies + near_copies + ends:
        copy.wait_send()

    @pl.when(at_edge)
    def _():
        for copy in rotor_copies:
            copy.wait_send()


def on_device(basis, jac_block, face_coef, panel_inverse, rotor_offset):
    total = basis.shape[1] * basis.shape[2] * basis.shape[3] * lax.axis_size(NAMES)
    row = jax.ShapeDtypeStruct((NC, 1, W), F32)
    any_space = pl.BlockSpec(memory_space=pl.ANY)
    vmem = pl.BlockSpec(memory_space=pltpu.VMEM)
    dma = pltpu.SemaphoreType.DMA
    phase_shapes = []
    for axes in PHASES:
        n = len(offsets_of(axes))
        phase_shapes += [
            pltpu.VMEM((1, W), F32),
            pltpu.VMEM(((n + 7) // 8 * 8, W), F32),
            dma,
            dma,
        ]
    precond, v, hess = pl.pallas_call(
        functools.partial(kernel, float(total)),
        out_shape=(row, row, jax.ShapeDtypeStruct((1, W), F32)),
        in_specs=[any_space] * 5,
        out_specs=(vmem,) * 3,
        scratch_shapes=[
            pltpu.VMEM((KB, 8, W), F32),
            pltpu.VMEM((NC, 8, W), F32),
            pltpu.VMEM((4, 8, W), F32),
            pltpu.VMEM((2, 320, 640), jnp.bfloat16),
            pltpu.SMEM((1,), jnp.int32),
            pltpu.VMEM((8, W), F32),
            pltpu.VMEM((2, 8, W), F32),
            pltpu.VMEM((320, 640), jnp.bfloat16),
            pltpu.VMEM((320, 640), jnp.bfloat16),
            pltpu.VMEM((8, W), F32),
            pltpu.VMEM((4, 8, W), F32),
            pltpu.VMEM((3, 8, W), F32),
            pltpu.VMEM((8, W), F32),
            dma((15,)),
            dma((2,)),
            dma((2,)),
            dma((4,)),
            dma((4,)),
            dma((3,)),
            dma((3,)),
            *phase_shapes,
        ],
        compiler_params=pltpu.CompilerParams(collective_id=0, has_side_effects=True),
        name="schwarz_step",
    )(basis, jac_block, face_coef, panel_inverse, rotor_offset)
    return precond, v, hess[0, : KB + 1]


def solution(mesh):
    finer = Mesh(mesh.devices.reshape(4, 8, 2, 8, 2), NAMES)
    in_specs = (
        P(None, None, BAND, THETA),
        P(None, None, BAND, THETA),
        P(None, None, BAND, THETA),
        P(BAND, THETA, None, None),
        P(),
    )
    out_specs = (P(None, BAND, THETA), P(None, BAND, THETA), P())
    return jax.shard_map(
        on_device, mesh=finer, in_specs=in_specs, out_specs=out_specs, check_vma=False
    )
```

```python
import functools
import itertools

import jax
import jax.numpy as jnp
from jax import lax
from jax.experimental import pallas as pl
from jax.experimental.pallas import tpu as pltpu
from jax.sharding import Mesh
from jax.sharding import PartitionSpec as P

THETA = ("theta_0", "theta_1", "theta_2")
BAND = ("band_0", "band_1")
NAMES = ("theta_0", "theta_1", "theta_2", "band_0", "band_1")
MESH = pl.DeviceIdType.MESH

SIZES = {"x": 8, "y": 8, "z": 8, "c": 2}
PHASES = (("x", "y"), ("z", "c"))
F32 = jnp.float32
KB, NC, W = 4, 5, 128
PAIRS = [(a, b) for a in range(KB) for b in range(a, KB)]
IMG = KB + len(PAIRS)


def ring_distance(d, n):
    return min(d, n - d)


def offsets_of(axes):
    every = itertools.product(*[range(SIZES[a]) for a in axes])
    some = [o for o in every if any(o)]
    return sorted(
        some, key=lambda o: -sum(ring_distance(d, SIZES[a]) for d, a in zip(o, axes))
    )


def add_mod(v, d, n):
    if d == 0:
        return v
    s = v + d
    return jnp.where(s >= n, s - n, s)


def moved(here, axes, offset):
    t0, z, c, y, xl = here
    for a, d in zip(axes, offset):
        if d == 0:
            continue
        if a == "x":
            if d % 2:
                s = t0 + xl + d // 2
                t0 = jnp.where(s >= 4, s - 4, s)
                xl = 1 - xl
            else:
                t0 = add_mod(t0, d // 2, 4)
        elif a == "y":
            y = add_mod(y, d, 8)
        elif a == "z":
            z = add_mod(z, d, 8)
        else:
            c = 1 - c
    return (t0, z, c, y, xl)


def theta_next(here):
    t0, z, c, y, xl = here
    z1 = z + c
    over = z1 >= 8
    t1 = jnp.where(over, t0 + 1, t0)
    return (jnp.where(t1 >= 4, t1 - 4, t1), jnp.where(over, 0, z1), 1 - c, y, xl)


def theta_prev(here):
    t0, z, c, y, xl = here
    z1 = z - 1 + c
    under = z1 < 0
    t1 = jnp.where(under, t0 - 1, t0)
    return (jnp.where(t1 < 0, t1 + 4, t1), jnp.where(under, 7, z1), 1 - c, y, xl)


def band_next(here):
    t0, z, c, y, xl = here
    y1 = y + xl
    return (t0, z, c, jnp.where(y1 >= 8, y1 - 8, y1), 1 - xl)


def band_prev(here):
    t0, z, c, y, xl = here
    y1 = y - 1 + xl
    return (t0, z, c, jnp.where(y1 < 0, y1 + 8, y1), 1 - xl)


def across(here):
    t0, z, c, y, xl = here
    return (add_mod(t0, 2, 4), z, c, 7 - y, 1 - xl)


def kernel(
    total,
    basis_hbm,
    jac_hbm,
    face_hbm,
    pinv_hbm,
    off,
    image_buf,
    prec,
    line_out,
    basis,
    jac,
    face,
    pinv,
    mine,
    halo,
    bown,
    bhalo,
    near,
    rotor,
    met,
    load_sems,
    halo_send,
    halo_recv,
    near_send,
    near_recv,
    rotor_send,
    rotor_recv,
    *phase_refs,
):
    here = tuple(lax.axis_index(n) for n in NAMES)
    t0, z, c, y, xl = here
    band = y * 2 + xl
    at_edge = (band == 7) | (band == 8)
    left, right = theta_prev(here), theta_next(here)
    below, above = band_prev(here), band_next(here)
    opposite = across(here)
    opposite3 = (theta_prev(opposite), opposite, theta_next(opposite))

    loads = []
    zero3 = jnp.zeros((3, W), F32)
    for i in range(KB):
        loads.append((basis_hbm.at[i, :, 0, :], basis.at[i, pl.ds(0, NC), :], 0 if i == KB - 1 else 1))
    for w in range(NC):
        loads.append((jac_hbm.at[:, w, 0, :], jac.at[w, pl.ds(0, NC), :], 1))
    for d in range(4):
        loads.append((face_hbm.at[d, :, 0, :], face.at[d, pl.ds(0, NC), :], 1))
    copies = [
        pltpu.make_async_copy(src, dst, load_sems.at[k]) for k, (src, dst, _) in enumerate(loads)
    ]
    copies[KB - 1].start()
    pinv_copy = pltpu.make_async_copy(pinv_hbm.at[0], pinv, load_sems.at[len(loads)])
    pinv_copy.start()
    for k, copy in enumerate(copies):
        if k != KB - 1:
            copy.start()

    barrier = pltpu.get_barrier_semaphore()
    ones = [(a, o) for a in "xyz" for o in (1, 7)]
    steps = [moved(here, (a,), (o,)) for a, o in ones]
    partners = [left, right, below, above] + steps
    for p in partners:
        pl.semaphore_signal(barrier, inc=1, device_id=p, device_id_type=MESH)

    def tell(k, devices):
        for p in devices:
            pl.semaphore_signal(met.at[k], inc=1, device_id=p, device_id_type=MESH)

    for i in range(KB):
        basis[i, NC:, :] = zero3
    for w in range(NC):
        jac[w, NC:, :] = zero3
    for d in range(4):
        face[d, NC:, :] = zero3

    lane = lax.broadcasted_iota(jnp.int32, (8, W), 1)
    row = lax.broadcasted_iota(jnp.int32, (8, W), 0)

    copies[KB - 1].wait()
    own = pltpu.roll(basis[KB - 1].astype(jnp.bfloat16).astype(F32), W // 2, 1)
    mine[...] = own

    pl.semaphore_wait(barrier, len(partners))
    halo_copies = []
    for k, p in enumerate((left, right)):
        copy = pltpu.make_async_remote_copy(
            mine, halo.at[1 - k], halo_send.at[k], halo_recv.at[1 - k],
            device_id=p, device_id_type=MESH,
        )
        copy.start()
        halo_copies.append(copy)
    tell(0, steps)

    pinv_copy.wait()
    cols = lax.broadcasted_iota(jnp.int32, (320, 640), 1) % W
    a0, a1 = pinv[0], pinv[1]
    bown[...] = jnp.where(cols < W // 2, a1, a0)
    bhalo[...] = jnp.where(cols < W // 2, a0, a1)
    xrow = lax.broadcasted_iota(jnp.int32, (W, W), 0)
    xlane = lax.broadcasted_iota(jnp.int32, (W, W), 1)
    same = (xrow < W // 2) == (xlane < W // 2)

    def spread(vec, keep):
        parts = [
            jnp.where(keep, jnp.broadcast_to(vec[u : u + 1, :], (W, W)), 0.0).astype(jnp.bfloat16)
            for u in range(NC)
        ]
        return jnp.concatenate(parts, axis=1)

    def times(mat, rhs):
        return lax.dot_general(
            mat, rhs, (((1,), (1,)), ((), ())), preferred_element_type=F32
        )

    r_own = times(bown[...], spread(own, jnp.logical_not(same)))
    pick = lax.broadcasted_iota(jnp.int32, (64, W), 0) == lax.broadcasted_iota(
        jnp.int32, (64, W), 1
    ) % 64

    def fold(r):
        return [
            jnp.sum(jnp.where(pick, r[u * 64 : (u + 1) * 64, :], 0.0), axis=0, keepdims=True)
            for u in range(NC)
        ]

    own_part = fold(r_own)

    pl.semaphore_wait(met.at[0], len(steps))
    twos = [moved(here, (a,), (2 if o == 1 else 6,)) for a, o in ones]
    tell(1, twos)

    for k, copy in enumerate(copies):
        if k != KB - 1:
            copy.wait()

    gram_rows = [jnp.sum(basis[a] * basis[b], axis=0, keepdims=True) for a, b in PAIRS]
    gram_rows += [jnp.zeros((1, W), F32)] * (16 - len(PAIRS))
    gram_sum = jnp.sum(jnp.concatenate(gram_rows, axis=0), axis=1, keepdims=True)
    lane16 = lax.broadcasted_iota(jnp.int32, (16, W), 1)
    row16 = lax.broadcasted_iota(jnp.int32, (16, W), 0)
    gram_line = jnp.sum(jnp.where(lane16 == row16 + KB, gram_sum, 0.0), axis=0, keepdims=True)
    gram_line = jnp.where(lane16[:1] < IMG, gram_line, 0.0)

    for k, copy in enumerate(halo_copies):
        copy.wait_recv()
    ph = jnp.where(lane < W // 2, halo[0], halo[1])
    halo_part = fold(times(bhalo[...], spread(ph, same)))
    zero1 = jnp.zeros((1, W), F32)
    pre = jnp.concatenate([a + b for a, b in zip(own_part, halo_part)] + [zero1] * 3, axis=0)
    prec[...] = pre

    near_copies = []
    for slot, p in ((3, below), (2, above), (1, left), (0, right)):
        copy = pltpu.make_async_remote_copy(
            prec, near.at[slot], near_send.at[slot], near_recv.at[slot],
            device_id=p, device_id_type=MESH,
        )
        near_copies.append(copy)
    rotor_copies = []
    for k in range(3):
        rotor_copies.append(
            pltpu.make_async_remote_copy(
                prec, rotor.at[2 - k], rotor_send.at[k], rotor_recv.at[2 - k],
                device_id=opposite3[k], device_id_type=MESH,
            )
        )

    for copy in near_copies:
        copy.start()

    pl.semaphore_wait(met.at[1], len(twos))
    tell(2, (left, right))
    column = [moved(here, ("y",), (d,)) for d in (4, 3, 5, 2, 6, 1, 7)]
    tell(3, column)

    base = 6.0 * pre
    for w in range(NC):
        base = base + jac[w] * pre[w : w + 1, :]

    pl.semaphore_wait(met.at[2], 2)

    @pl.when(at_edge)
    def _():
        for copy in rotor_copies:
            copy.start()

    for copy in near_copies:
        copy.wait_recv()
    tm = pltpu.roll(jnp.where(lane == W - 1, near[0], pre), 1, 1)
    tp = pltpu.roll(jnp.where(lane == 0, near[1], pre), W - 1, 1)
    base = base - face[0] * tm - face[1] * tp
    image_buf[...] = base
    near[2] = jnp.where(band == 0, 0.0, near[2])
    near[3] = jnp.where(band == 15, 0.0, near[3])

    @pl.when(at_edge)
    def _():
        for copy in rotor_copies:
            copy.wait_recv()
        shift = off[0] - 4032
        o = jnp.where(band == 7, shift, W - shift)
        joined = jnp.where(
            lane >= 64 + o, rotor[0], jnp.where(lane < o - 64, rotor[2], rotor[1])
        )
        turn = 64 - o
        turn = jnp.where(turn < 0, turn + W, turn)
        crossed = pltpu.roll(joined, turn, 1)
        near[2] = jnp.where(band == 8, crossed, near[2])
        near[3] = jnp.where(band == 7, crossed, near[3])

    pl.semaphore_wait(met.at[3], len(column))

    image = image_buf[...] - face[2] * near[2] - face[3] * near[3]
    image_buf[...] = image

    late = [jnp.sum(basis[i] * image, axis=0, keepdims=True) for i in range(KB)]
    late.append(jnp.sum(image * image, axis=0, keepdims=True))
    late += [zero1] * 3
    late_sum = jnp.sum(jnp.concatenate(late, axis=0), axis=1, keepdims=True)
    want = jnp.where(row < KB, row, IMG)
    want = jnp.where(row > KB, -1, want)
    line = gram_line + jnp.sum(jnp.where(lane == want, late_sum, 0.0), axis=0, keepdims=True)

    ends = []
    for k, axes in enumerate(PHASES):
        src, slots, ssem, rsem = phase_refs[4 * k : 4 * k + 4]
        some = offsets_of(axes)
        n = len(some)
        src[...] = line
        for s, o in enumerate(some):
            pltpu.make_async_remote_copy(
                src, slots.at[pl.ds(s, 1), :], ssem, rsem,
                device_id=moved(here, axes, o), device_id_type=MESH,
            ).start()
        everything = slots.at[pl.ds(0, n), :]
        whole = pltpu.make_async_remote_copy(
            everything, everything, ssem, rsem, device_id=right, device_id_type=MESH
        )
        whole.wait_recv()
        ends.append(whole)
        line = line + jnp.sum(slots[pl.ds(0, n), :], axis=0, keepdims=True)

    line_out[...] = line

    for copy in halo_copies + near_copies + ends:
        copy.wait_send()

    @pl.when(at_edge)
    def _():
        for copy in rotor_copies:
            copy.wait_send()


def finish(total, image, prec, line_in, basis, precond_out, v_out, hess_out):
    line = line_in[...] * (1.0 / total)
    lane16 = lax.broadcasted_iota(jnp.int32, (16, W), 1)
    row16 = lax.broadcasted_iota(jnp.int32, (16, W), 0)
    spread16 = jnp.sum(jnp.where(lane16 == row16, line, 0.0), axis=1, keepdims=True)
    at = [jnp.broadcast_to(spread16[i : i + 1, :], (1, W)) for i in range(IMG + 1)]
    proj = at[:KB]
    gram = {pair: at[KB + k] for k, pair in enumerate(PAIRS)}
    squares = at[IMG]
    ortho = image[...]
    for i in range(KB):
        squares = squares - 2.0 * proj[i] * proj[i]
        ortho = ortho - proj[i] * basis[i]
    for (a, b), g in gram.items():
        term = proj[a] * g * proj[b]
        squares = squares + (term if a == b else 2.0 * term)
    hnorm = jnp.sqrt(squares + 1e-06)
    v = ortho / hnorm
    for u in range(NC):
        precond_out[u] = prec[u : u + 1, :]
        v_out[u] = v[u : u + 1, :]
    hess_out[...] = jnp.where(lane16[:1] < KB, line, hnorm)[0, : KB + 1]


def on_device(basis, jac_block, face_coef, panel_inverse, rotor_offset):
    total = basis.shape[1] * basis.shape[2] * basis.shape[3] * lax.axis_size(NAMES)
    row = jax.ShapeDtypeStruct((NC, 1, W), F32)
    arrays = (basis, jac_block, face_coef, panel_inverse)
    vmem = pl.BlockSpec(memory_space=pltpu.VMEM)
    dma = pltpu.SemaphoreType.DMA
    phase_shapes = []
    for axes in PHASES:
        n = len(offsets_of(axes))
        phase_shapes += [
            pltpu.VMEM((1, W), F32),
            pltpu.VMEM(((n + 7) // 8 * 8, W), F32),
            dma,
            dma,
        ]
    tile = jax.ShapeDtypeStruct((8, W), F32)
    hbm = pl.BlockSpec(memory_space=pltpu.HBM)
    image, precond, line, basis_tiles = pl.pallas_call(
        functools.partial(kernel, float(total)),
        out_shape=(
            tile,
            tile,
            jax.ShapeDtypeStruct((1, W), F32),
            jax.ShapeDtypeStruct((KB, 8, W), F32),
        ),
        in_specs=[hbm] * 4 + [pl.BlockSpec(memory_space=pltpu.SMEM)],
        out_specs=(vmem,) * 4,
        scratch_shapes=[
            pltpu.VMEM((NC, 8, W), F32),
            pltpu.VMEM((4, 8, W), F32),
            pltpu.VMEM((2, 320, 640), jnp.bfloat16),
            pltpu.VMEM((8, W), F32),
            pltpu.VMEM((2, 8, W), F32),
            pltpu.VMEM((320, 640), jnp.bfloat16),
            pltpu.VMEM((320, 640), jnp.bfloat16),
            pltpu.VMEM((4, 8, W), F32),
            pltpu.VMEM((3, 8, W), F32),
            pltpu.SemaphoreType.REGULAR((4,)),
            dma((14,)),
            dma((2,)),
            dma((2,)),
            dma((4,)),
            dma((4,)),
            dma((3,)),
            dma((3,)),
            *phase_shapes,
        ],
        compiler_params=pltpu.CompilerParams(
            collective_id=0, has_side_effects=True, vmem_limit_bytes=8 << 20
        ),
        name="schwarz_step",
    )(*[pltpu.with_memory_space_constraint(a, pltpu.HBM) for a in arrays], rotor_offset)
    return pl.pallas_call(
        functools.partial(finish, float(total)),
        out_shape=(row, row, jax.ShapeDtypeStruct((KB + 1,), F32)),
        in_specs=[vmem] * 4,
        out_specs=(vmem,) * 3,
        compiler_params=pltpu.CompilerParams(vmem_limit_bytes=4 << 20),
        name="schwarz_finish",
    )(image, precond, line, basis_tiles)


def solution(mesh):
    finer = Mesh(mesh.devices.reshape(4, 8, 2, 8, 2), NAMES)
    in_specs = (
        P(None, None, BAND, THETA),
        P(None, None, BAND, THETA),
        P(None, None, BAND, THETA),
        P(BAND, THETA, None, None),
        P(),
    )
    out_specs = (P(None, BAND, THETA), P(None, BAND, THETA), P())
    return jax.shard_map(
        on_device, mesh=finer, in_specs=in_specs, out_specs=out_specs, check_vma=False
    )
```

```python
import functools
import itertools

import jax
import jax.numpy as jnp
from jax import lax
from jax.experimental import pallas as pl
from jax.experimental.pallas import tpu as pltpu
from jax.sharding import Mesh
from jax.sharding import PartitionSpec as P

THETA = ("theta_0", "theta_1", "theta_2")
BAND = ("band_0", "band_1")
NAMES = ("theta_0", "theta_1", "theta_2", "band_0", "band_1")
MESH = pl.DeviceIdType.MESH

SIZES = {"x": 8, "y": 8, "z": 8, "c": 2}
PHASES = (("z", "c"), ("x", "y"))
F32 = jnp.float32
KB, NC, W = 4, 5, 128
PAIRS = [(a, b) for a in range(KB) for b in range(a, KB)]
IMG = KB + len(PAIRS)


def ring_distance(d, n):
    return min(d, n - d)


def offsets_of(axes):
    every = itertools.product(*[range(SIZES[a]) for a in axes])
    some = [o for o in every if any(o)]
    return sorted(
        some, key=lambda o: -sum(ring_distance(d, SIZES[a]) for d, a in zip(o, axes))
    )


def add_mod(v, d, n):
    if d == 0:
        return v
    s = v + d
    return jnp.where(s >= n, s - n, s)


def moved(here, axes, offset):
    t0, z, c, y, xl = here
    for a, d in zip(axes, offset):
        if d == 0:
            continue
        if a == "x":
            if d % 2:
                s = t0 + xl + d // 2
                t0 = jnp.where(s >= 4, s - 4, s)
                xl = 1 - xl
            else:
                t0 = add_mod(t0, d // 2, 4)
        elif a == "y":
            y = add_mod(y, d, 8)
        elif a == "z":
            z = add_mod(z, d, 8)
        else:
            c = 1 - c
    return (t0, z, c, y, xl)


def theta_next(here):
    t0, z, c, y, xl = here
    z1 = z + c
    over = z1 >= 8
    t1 = jnp.where(over, t0 + 1, t0)
    return (jnp.where(t1 >= 4, t1 - 4, t1), jnp.where(over, 0, z1), 1 - c, y, xl)


def theta_prev(here):
    t0, z, c, y, xl = here
    z1 = z - 1 + c
    under = z1 < 0
    t1 = jnp.where(under, t0 - 1, t0)
    return (jnp.where(t1 < 0, t1 + 4, t1), jnp.where(under, 7, z1), 1 - c, y, xl)


def band_next(here):
    t0, z, c, y, xl = here
    y1 = y + xl
    return (t0, z, c, jnp.where(y1 >= 8, y1 - 8, y1), 1 - xl)


def band_prev(here):
    t0, z, c, y, xl = here
    y1 = y - 1 + xl
    return (t0, z, c, jnp.where(y1 < 0, y1 + 8, y1), 1 - xl)


def across(here):
    t0, z, c, y, xl = here
    return (add_mod(t0, 2, 4), z, c, 7 - y, 1 - xl)


def kernel(
    total,
    basis_hbm,
    jac_hbm,
    face_hbm,
    pinv_hbm,
    off,
    image_buf,
    prec,
    line_out,
    basis,
    jac,
    face,
    pinv,
    mine,
    halo,
    edge_out,
    edge_in,
    bown,
    bhalo,
    near,
    rotor,
    met,
    load_sems,
    halo_send,
    halo_recv,
    edge_send,
    edge_recv,
    near_send,
    near_recv,
    rotor_send,
    rotor_recv,
    *phase_refs,
):
    here = tuple(lax.axis_index(n) for n in NAMES)
    t0, z, c, y, xl = here
    band = y * 2 + xl
    at_edge = (band == 7) | (band == 8)
    has_low = (band != 0) & (band != 8)
    has_high = (band != 7) & (band != 15)
    left, right = theta_prev(here), theta_next(here)
    below, above = band_prev(here), band_next(here)
    opposite = across(here)
    opposite3 = (theta_prev(opposite), opposite, theta_next(opposite))

    loads = []
    zero3 = jnp.zeros((3, W), F32)
    for i in range(KB):
        loads.append((basis_hbm.at[i, :, 0, :], basis.at[i, pl.ds(0, NC), :], 0 if i == KB - 1 else 1))
    for w in range(NC):
        loads.append((jac_hbm.at[:, w, 0, :], jac.at[w, pl.ds(0, NC), :], 1))
    for d in range(4):
        loads.append((face_hbm.at[d, :, 0, :], face.at[d, pl.ds(0, NC), :], 1))
    copies = [
        pltpu.make_async_copy(src, dst, load_sems.at[k]) for k, (src, dst, _) in enumerate(loads)
    ]
    copies[KB - 1].start()
    pinv_copy = pltpu.make_async_copy(pinv_hbm.at[0], pinv, load_sems.at[len(loads)])
    pinv_copy.start()
    for k, copy in enumerate(copies):
        if k != KB - 1:
            copy.start()

    barrier = pltpu.get_barrier_semaphore()
    ones = [(a, o) for a in "xyz" for o in (1, 7)]
    steps = [moved(here, (a,), (o,)) for a, o in ones]
    partners = [left, right, below, above] + steps
    for p in partners:
        pl.semaphore_signal(barrier, inc=1, device_id=p, device_id_type=MESH)

    @pl.when(band == 7)
    def _():
        for p in opposite3:
            pl.semaphore_signal(barrier, inc=1, device_id=p, device_id_type=MESH)

    def tell(k, devices):
        for p in devices:
            pl.semaphore_signal(met.at[k], inc=1, device_id=p, device_id_type=MESH)

    for i in range(KB):
        basis[i, NC:, :] = zero3
    for w in range(NC):
        jac[w, NC:, :] = zero3
    for d in range(4):
        face[d, NC:, :] = zero3

    lane = lax.broadcasted_iota(jnp.int32, (8, W), 1)
    row = lax.broadcasted_iota(jnp.int32, (8, W), 0)

    pl.semaphore_wait(barrier, len(partners) + jnp.where(band == 8, 3, 0))

    @pl.when(band == 8)
    def _():
        tell(4, opposite3)

    tell(0, steps)

    copies[KB - 1].wait()
    own = pltpu.roll(basis[KB - 1].astype(jnp.bfloat16).astype(F32), W // 2, 1)
    mine[...] = own

    to_left = pltpu.make_async_remote_copy(
        mine, halo.at[1], halo_send.at[0], halo_recv.at[1], device_id=left, device_id_type=MESH
    )
    to_right = pltpu.make_async_remote_copy(
        mine, halo.at[0], halo_send.at[1], halo_recv.at[0], device_id=right, device_id_type=MESH
    )
    edge_left = pltpu.make_async_remote_copy(
        edge_out.at[0], edge_in.at[1], edge_send.at[0], edge_recv.at[1],
        device_id=left, device_id_type=MESH,
    )
    edge_right = pltpu.make_async_remote_copy(
        edge_out.at[1], edge_in.at[0], edge_send.at[1], edge_recv.at[0],
        device_id=right, device_id_type=MESH,
    )
    to_right.start()

    to_left.start()

    pinv_copy.wait()

    def rows_of(side, k):
        some = [pinv[side, u * 64 + k : u * 64 + k + 1, :].astype(F32) for u in range(NC)]
        return jnp.concatenate(some + [jnp.zeros((3, 640), F32)], axis=0).astype(jnp.bfloat16)

    edge_out[0] = rows_of(0, 0)
    edge_out[1] = rows_of(1, 63)
    edge_right.start()

    edge_left.start()

    cols = lax.broadcasted_iota(jnp.int32, (320, 640), 1) % W
    a0, a1 = pinv[0], pinv[1]
    bown[...] = jnp.where(cols < W // 2, a1, a0)
    bhalo[...] = jnp.where(cols < W // 2, a0, a1)
    xrow = lax.broadcasted_iota(jnp.int32, (W, W), 0)
    xlane = lax.broadcasted_iota(jnp.int32, (W, W), 1)
    same = (xrow < W // 2) == (xlane < W // 2)

    def spread(vec, keep):
        parts = [
            jnp.where(keep, jnp.broadcast_to(vec[u : u + 1, :], (W, W)), 0.0).astype(jnp.bfloat16)
            for u in range(NC)
        ]
        return jnp.concatenate(parts, axis=1)

    def times(mat, rhs):
        return lax.dot_general(
            mat, rhs, (((1,), (1,)), ((), ())), preferred_element_type=F32
        )

    r_own = times(bown[...], spread(own, jnp.logical_not(same)))
    pick = lax.broadcasted_iota(jnp.int32, (64, W), 0) == lax.broadcasted_iota(
        jnp.int32, (64, W), 1
    ) % 64

    def fold(r):
        return [
            jnp.sum(jnp.where(pick, r[u * 64 : (u + 1) * 64, :], 0.0), axis=0, keepdims=True)
            for u in range(NC)
        ]

    own_part = fold(r_own)

    pl.semaphore_wait(met.at[0], len(steps))
    twos = [moved(here, (a,), (2 if o == 1 else 6,)) for a, o in ones]
    tell(1, twos)

    for k, copy in enumerate(copies):
        if k != KB - 1:
            copy.wait()

    gram_rows = [jnp.sum(basis[a] * basis[b], axis=0, keepdims=True) for a, b in PAIRS]
    gram_rows += [jnp.zeros((1, W), F32)] * (16 - len(PAIRS))
    gram_sum = jnp.sum(jnp.concatenate(gram_rows, axis=0), axis=1, keepdims=True)
    lane16 = lax.broadcasted_iota(jnp.int32, (16, W), 1)
    row16 = lax.broadcasted_iota(jnp.int32, (16, W), 0)
    gram_line = jnp.sum(jnp.where(lane16 == row16 + KB, gram_sum, 0.0), axis=0, keepdims=True)
    gram_line = jnp.where(lane16[:1] < IMG, gram_line, 0.0)

    to_right.wait_recv()
    to_left.wait_recv()
    ph = jnp.where(lane < W // 2, halo[0], halo[1])
    halo_part = fold(times(bhalo[...], spread(ph, same)))
    zero1 = jnp.zeros((1, W), F32)
    pre = jnp.concatenate([a + b for a, b in zip(own_part, halo_part)] + [zero1] * 3, axis=0)
    prec[...] = pre

    to_low = pltpu.make_async_remote_copy(
        prec, near.at[1], near_send.at[0], near_recv.at[1], device_id=below, device_id_type=MESH
    )
    to_high = pltpu.make_async_remote_copy(
        prec, near.at[0], near_send.at[1], near_recv.at[0], device_id=above, device_id_type=MESH
    )

    @pl.when(has_low)
    def _():
        to_low.start()

    @pl.when(has_high)
    def _():
        to_high.start()

    rotor_copies = []
    for k in range(3):
        rotor_copies.append(
            pltpu.make_async_remote_copy(
                prec, rotor.at[2 - k], rotor_send.at[k], rotor_recv.at[2 - k],
                device_id=opposite3[k], device_id_type=MESH,
            )
        )

    @pl.when(band == 7)
    def _():
        pl.semaphore_wait(met.at[4], 3)

    @pl.when(at_edge)
    def _():
        for copy in rotor_copies:
            copy.start()

    pl.semaphore_wait(met.at[1], len(twos))
    tell(2, [(t0, z, 1 - c, y, xl)])
    column = [moved(here, ("y",), (d,)) for d in (4, 3, 5, 2, 6, 1, 7)]
    tell(3, column)

    edge_right.wait_recv()
    edge_left.wait_recv()
    panel0 = jnp.where(lane < W // 2, ph, own)
    panel1 = jnp.where(lane < W // 2, own, ph)

    def edge_of(side, panel):
        rows = edge_in[side].astype(F32)
        total_row = rows[:, :W] * panel[0:1, :]
        for u in range(1, NC):
            total_row = total_row + rows[:, u * W : (u + 1) * W] * panel[u : u + 1, :]
        return jnp.sum(total_row, axis=1, keepdims=True)

    tm = jnp.where(lane == 0, edge_of(0, panel0), pltpu.roll(pre, 1, 1))
    tp = jnp.where(lane == W - 1, edge_of(1, panel1), pltpu.roll(pre, W - 1, 1))
    base = 6.0 * pre - face[0] * tm - face[1] * tp
    for w in range(NC):
        base = base + jac[w] * pre[w : w + 1, :]
    image_buf[...] = base

    @pl.when(has_low)
    def _():
        to_high.wait_recv()

    @pl.when(has_high)
    def _():
        to_low.wait_recv()

    @pl.when(band == 0)
    def _():
        near[0] = jnp.zeros((8, W), F32)

    @pl.when(band == 15)
    def _():
        near[1] = jnp.zeros((8, W), F32)

    @pl.when(at_edge)
    def _():
        for copy in rotor_copies:
            copy.wait_recv()
        shift = off[0] - 4032
        o = jnp.where(band == 7, shift, W - shift)
        joined = jnp.where(
            lane >= 64 + o, rotor[0], jnp.where(lane < o - 64, rotor[2], rotor[1])
        )
        turn = 64 - o
        turn = jnp.where(turn < 0, turn + W, turn)
        crossed = pltpu.roll(joined, turn, 1)

        @pl.when(band == 8)
        def _():
            near[0] = crossed

        @pl.when(band == 7)
        def _():
            near[1] = crossed


    pl.semaphore_wait(met.at[2], 1)

    image = image_buf[...] - face[2] * near[0] - face[3] * near[1]
    image_buf[...] = image

    late = [jnp.sum(basis[i] * image, axis=0, keepdims=True) for i in range(KB)]
    late.append(jnp.sum(image * image, axis=0, keepdims=True))
    late += [zero1] * 3
    late_sum = jnp.sum(jnp.concatenate(late, axis=0), axis=1, keepdims=True)
    want = jnp.where(row < KB, row, IMG)
    want = jnp.where(row > KB, -1, want)
    line = gram_line + jnp.sum(jnp.where(lane == want, late_sum, 0.0), axis=0, keepdims=True)

    ends = []
    for k, axes in enumerate(PHASES):
        src, slots, ssem, rsem = phase_refs[4 * k : 4 * k + 4]
        some = offsets_of(axes)
        n = len(some)
        src[...] = line
        if k == 1:
            pl.semaphore_wait(met.at[3], len(column))
        for s, o in enumerate(some):
            pltpu.make_async_remote_copy(
                src, slots.at[pl.ds(s, 1), :], ssem, rsem,
                device_id=moved(here, axes, o), device_id_type=MESH,
            ).start()
        everything = slots.at[pl.ds(0, n), :]
        whole = pltpu.make_async_remote_copy(
            everything, everything, ssem, rsem, device_id=right, device_id_type=MESH
        )
        whole.wait_recv()
        ends.append(whole)
        line = line + jnp.sum(slots[pl.ds(0, n), :], axis=0, keepdims=True)

    line_out[...] = line

    for copy in [to_left, to_right, edge_left, edge_right] + ends:
        copy.wait_send()

    @pl.when(has_low)
    def _():
        to_low.wait_send()

    @pl.when(has_high)
    def _():
        to_high.wait_send()

    @pl.when(at_edge)
    def _():
        for copy in rotor_copies:
            copy.wait_send()


def finish(total, image, prec, line_in, basis, precond_out, v_out, hess_out):
    line = line_in[...] * (1.0 / total)
    lane16 = lax.broadcasted_iota(jnp.int32, (16, W), 1)
    row16 = lax.broadcasted_iota(jnp.int32, (16, W), 0)
    spread16 = jnp.sum(jnp.where(lane16 == row16, line, 0.0), axis=1, keepdims=True)
    at = [jnp.broadcast_to(spread16[i : i + 1, :], (1, W)) for i in range(IMG + 1)]
    proj = at[:KB]
    gram = {pair: at[KB + k] for k, pair in enumerate(PAIRS)}
    squares = at[IMG]
    ortho = image[...]
    for i in range(KB):
        squares = squares - 2.0 * proj[i] * proj[i]
        ortho = ortho - proj[i] * basis[i]
    for (a, b), g in gram.items():
        term = proj[a] * g * proj[b]
        squares = squares + (term if a == b else 2.0 * term)
    hnorm = jnp.sqrt(squares + 1e-06)
    v = ortho / hnorm
    for u in range(NC):
        precond_out[u] = prec[u : u + 1, :]
        v_out[u] = v[u : u + 1, :]
    hess_out[...] = jnp.where(lane16[:1] < KB, line, hnorm)[0, : KB + 1]


def on_device(basis, jac_block, face_coef, panel_inverse, rotor_offset):
    total = basis.shape[1] * basis.shape[2] * basis.shape[3] * lax.axis_size(NAMES)
    row = jax.ShapeDtypeStruct((NC, 1, W), F32)
    arrays = (basis, jac_block, face_coef, panel_inverse)
    vmem = pl.BlockSpec(memory_space=pltpu.VMEM)
    dma = pltpu.SemaphoreType.DMA
    phase_shapes = []
    for axes in PHASES:
        n = len(offsets_of(axes))
        phase_shapes += [
            pltpu.VMEM((1, W), F32),
            pltpu.VMEM(((n + 7) // 8 * 8, W), F32),
            dma,
            dma,
        ]
    tile = jax.ShapeDtypeStruct((8, W), F32)
    hbm = pl.BlockSpec(memory_space=pltpu.HBM)
    image, precond, line, basis_tiles = pl.pallas_call(
        functools.partial(kernel, float(total)),
        out_shape=(
            tile,
            tile,
            jax.ShapeDtypeStruct((1, W), F32),
            jax.ShapeDtypeStruct((KB, 8, W), F32),
        ),
        in_specs=[hbm] * 4 + [pl.BlockSpec(memory_space=pltpu.SMEM)],
        out_specs=(vmem,) * 4,
        scratch_shapes=[
            pltpu.VMEM((NC, 8, W), F32),
            pltpu.VMEM((4, 8, W), F32),
            pltpu.VMEM((2, 320, 640), jnp.bfloat16),
            pltpu.VMEM((8, W), F32),
            pltpu.VMEM((2, 8, W), F32),
            pltpu.VMEM((2, 8, 640), jnp.bfloat16),
            pltpu.VMEM((2, 8, 640), jnp.bfloat16),
            pltpu.VMEM((320, 640), jnp.bfloat16),
            pltpu.VMEM((320, 640), jnp.bfloat16),
            pltpu.VMEM((2, 8, W), F32),
            pltpu.VMEM((3, 8, W), F32),
            pltpu.SemaphoreType.REGULAR((5,)),
            dma((14,)),
            dma((2,)),
            dma((2,)),
            dma((2,)),
            dma((2,)),
            dma((2,)),
            dma((2,)),
            dma((3,)),
            dma((3,)),
            *phase_shapes,
        ],
        compiler_params=pltpu.CompilerParams(
            collective_id=0, has_side_effects=True, vmem_limit_bytes=8 << 20
        ),
        name="schwarz_step",
    )(*[pltpu.with_memory_space_constraint(a, pltpu.HBM) for a in arrays], rotor_offset)
    return pl.pallas_call(
        functools.partial(finish, float(total)),
        out_shape=(row, row, jax.ShapeDtypeStruct((KB + 1,), F32)),
        in_specs=[vmem] * 4,
        out_specs=(vmem,) * 3,
        compiler_params=pltpu.CompilerParams(vmem_limit_bytes=4 << 20),
        name="schwarz_finish",
    )(image, precond, line, basis_tiles)


def solution(mesh):
    finer = Mesh(mesh.devices.reshape(4, 8, 2, 8, 2), NAMES)
    in_specs = (
        P(None, None, BAND, THETA),
        P(None, None, BAND, THETA),
        P(None, None, BAND, THETA),
        P(BAND, THETA, None, None),
        P(),
    )
    out_specs = (P(None, BAND, THETA), P(None, BAND, THETA), P())
    return jax.shard_map(
        on_device, mesh=finer, in_specs=in_specs, out_specs=out_specs, check_vma=False
    )
```

```python
import functools
import itertools

import jax
import jax.numpy as jnp
from jax import lax
from jax.experimental import pallas as pl
from jax.experimental.pallas import tpu as pltpu
from jax.sharding import Mesh
from jax.sharding import PartitionSpec as P

THETA = ("theta_0", "theta_1", "theta_2")
BAND = ("band_0", "band_1")
NAMES = ("theta_0", "theta_1", "theta_2", "band_0", "band_1")
MESH = pl.DeviceIdType.MESH

SIZES = {"x": 8, "y": 8, "z": 8, "c": 2}
PHASES = (("z", "c"), ("x", "y"))
F32 = jnp.float32
KB, NC, W = 4, 5, 128
PAIRS = [(a, b) for a in range(KB) for b in range(a, KB)]
IMG = KB + len(PAIRS)


def ring_distance(d, n):
    return min(d, n - d)


def offsets_of(axes):
    every = itertools.product(*[range(SIZES[a]) for a in axes])
    some = [o for o in every if any(o)]
    return sorted(
        some, key=lambda o: -sum(ring_distance(d, SIZES[a]) for d, a in zip(o, axes))
    )


def add_mod(v, d, n):
    if d == 0:
        return v
    s = v + d
    return jnp.where(s >= n, s - n, s)


def moved(here, axes, offset):
    t0, z, c, y, xl = here
    for a, d in zip(axes, offset):
        if d == 0:
            continue
        if a == "x":
            if d % 2:
                s = t0 + xl + d // 2
                t0 = jnp.where(s >= 4, s - 4, s)
                xl = 1 - xl
            else:
                t0 = add_mod(t0, d // 2, 4)
        elif a == "y":
            y = add_mod(y, d, 8)
        elif a == "z":
            z = add_mod(z, d, 8)
        else:
            c = 1 - c
    return (t0, z, c, y, xl)


def theta_next(here):
    t0, z, c, y, xl = here
    z1 = z + c
    over = z1 >= 8
    t1 = jnp.where(over, t0 + 1, t0)
    return (jnp.where(t1 >= 4, t1 - 4, t1), jnp.where(over, 0, z1), 1 - c, y, xl)


def theta_prev(here):
    t0, z, c, y, xl = here
    z1 = z - 1 + c
    under = z1 < 0
    t1 = jnp.where(under, t0 - 1, t0)
    return (jnp.where(t1 < 0, t1 + 4, t1), jnp.where(under, 7, z1), 1 - c, y, xl)


def band_next(here):
    t0, z, c, y, xl = here
    y1 = y + xl
    return (t0, z, c, jnp.where(y1 >= 8, y1 - 8, y1), 1 - xl)


def band_prev(here):
    t0, z, c, y, xl = here
    y1 = y - 1 + xl
    return (t0, z, c, jnp.where(y1 < 0, y1 + 8, y1), 1 - xl)


def across(here):
    t0, z, c, y, xl = here
    return (add_mod(t0, 2, 4), z, c, 7 - y, 1 - xl)


def kernel(
    total,
    basis_hbm,
    jac_hbm,
    face_hbm,
    pinv_hbm,
    off,
    image_buf,
    prec,
    line_out,
    basis,
    jac,
    face,
    pinv,
    mine,
    halo,
    edge_out,
    edge_in,
    bown,
    bhalo,
    near,
    rotor,
    met,
    load_sems,
    halo_send,
    halo_recv,
    edge_send,
    edge_recv,
    near_send,
    near_recv,
    rotor_send,
    rotor_recv,
    *phase_refs,
):
    here = tuple(lax.axis_index(n) for n in NAMES)
    t0, z, c, y, xl = here
    band = y * 2 + xl
    at_edge = (band == 7) | (band == 8)
    first = (z == 0) & (c == 0)
    has_low = (band != 0) & (band != 8)
    has_high = (band != 7) & (band != 15)
    left, right = theta_prev(here), theta_next(here)
    below, above = band_prev(here), band_next(here)
    opposite = across(here)
    opposite3 = (theta_prev(opposite), opposite, theta_next(opposite))

    loads = []
    zero3 = jnp.zeros((3, W), F32)
    for i in range(KB):
        loads.append((basis_hbm.at[i, :, 0, :], basis.at[i, pl.ds(0, NC), :], 0 if i == KB - 1 else 1))
    for w in range(NC):
        loads.append((jac_hbm.at[:, w, 0, :], jac.at[w, pl.ds(0, NC), :], 1))
    for d in range(4):
        loads.append((face_hbm.at[d, :, 0, :], face.at[d, pl.ds(0, NC), :], 1))
    copies = [
        pltpu.make_async_copy(src, dst, load_sems.at[k]) for k, (src, dst, _) in enumerate(loads)
    ]
    copies[KB - 1].start()
    pinv_copy = pltpu.make_async_copy(pinv_hbm.at[0], pinv, load_sems.at[len(loads)])
    pinv_copy.start()
    for k, copy in enumerate(copies):
        if k != KB - 1:
            copy.start()

    barrier = pltpu.get_barrier_semaphore()
    ones = [(a, o) for a in "xyz" for o in (1, 7)]
    steps = [moved(here, (a,), (o,)) for a, o in ones]
    partners = [left, right, below, above] + steps
    for p in partners:
        pl.semaphore_signal(barrier, inc=1, device_id=p, device_id_type=MESH)

    @pl.when(band == 7)
    def _():
        for p in opposite3:
            pl.semaphore_signal(barrier, inc=1, device_id=p, device_id_type=MESH)

    def tell(k, devices):
        for p in devices:
            pl.semaphore_signal(met.at[k], inc=1, device_id=p, device_id_type=MESH)

    for i in range(KB):
        basis[i, NC:, :] = zero3
    for w in range(NC):
        jac[w, NC:, :] = zero3
    for d in range(4):
        face[d, NC:, :] = zero3

    lane = lax.broadcasted_iota(jnp.int32, (8, W), 1)
    row = lax.broadcasted_iota(jnp.int32, (8, W), 0)

    pl.semaphore_wait(barrier, len(partners) + jnp.where(band == 8, 3, 0))

    @pl.when(band == 8)
    def _():
        for k in (1, 0, 2):
            tell(6 - k, [opposite3[k]])

    tell(0, steps)

    copies[KB - 1].wait()
    own = pltpu.roll(basis[KB - 1].astype(jnp.bfloat16).astype(F32), W // 2, 1)
    mine[...] = own

    to_left = pltpu.make_async_remote_copy(
        mine, halo.at[1], halo_send.at[0], halo_recv.at[1], device_id=left, device_id_type=MESH
    )
    to_right = pltpu.make_async_remote_copy(
        mine, halo.at[0], halo_send.at[1], halo_recv.at[0], device_id=right, device_id_type=MESH
    )
    edge_left = pltpu.make_async_remote_copy(
        edge_out.at[0], edge_in.at[1], edge_send.at[0], edge_recv.at[1],
        device_id=left, device_id_type=MESH,
    )
    edge_right = pltpu.make_async_remote_copy(
        edge_out.at[1], edge_in.at[0], edge_send.at[1], edge_recv.at[0],
        device_id=right, device_id_type=MESH,
    )
    to_right.start()

    to_left.start()

    pinv_copy.wait()

    def rows_of(side, k):
        some = [pinv[side, u * 64 + k : u * 64 + k + 1, :].astype(F32) for u in range(NC)]
        return jnp.concatenate(some + [jnp.zeros((3, 640), F32)], axis=0).astype(jnp.bfloat16)

    edge_out[0] = rows_of(0, 0)
    edge_out[1] = rows_of(1, 63)
    edge_right.start()

    edge_left.start()

    cols = lax.broadcasted_iota(jnp.int32, (320, 640), 1) % W
    a0, a1 = pinv[0], pinv[1]
    bown[...] = jnp.where(cols < W // 2, a1, a0)
    bhalo[...] = jnp.where(cols < W // 2, a0, a1)
    xrow = lax.broadcasted_iota(jnp.int32, (W, W), 0)
    xlane = lax.broadcasted_iota(jnp.int32, (W, W), 1)
    same = (xrow < W // 2) == (xlane < W // 2)

    def spread(vec, keep):
        parts = [
            jnp.where(keep, jnp.broadcast_to(vec[u : u + 1, :], (W, W)), 0.0).astype(jnp.bfloat16)
            for u in range(NC)
        ]
        return jnp.concatenate(parts, axis=1)

    def times(mat, rhs):
        return lax.dot_general(
            mat, rhs, (((1,), (1,)), ((), ())), preferred_element_type=F32
        )

    r_own = times(bown[...], spread(own, jnp.logical_not(same)))
    pick = lax.broadcasted_iota(jnp.int32, (64, W), 0) == lax.broadcasted_iota(
        jnp.int32, (64, W), 1
    ) % 64

    def fold(r):
        return [
            jnp.sum(jnp.where(pick, r[u * 64 : (u + 1) * 64, :], 0.0), axis=0, keepdims=True)
            for u in range(NC)
        ]

    own_part = fold(r_own)

    pl.semaphore_wait(met.at[0], len(steps))
    twos = [moved(here, (a,), (2 if o == 1 else 6,)) for a, o in ones]
    tell(1, twos)

    for k, copy in enumerate(copies):
        if k != KB - 1:
            copy.wait()

    gram_rows = [jnp.sum(basis[a] * basis[b], axis=0, keepdims=True) for a, b in PAIRS]
    gram_rows += [jnp.zeros((1, W), F32)] * (16 - len(PAIRS))
    gram_sum = jnp.sum(jnp.concatenate(gram_rows, axis=0), axis=1, keepdims=True)
    lane16 = lax.broadcasted_iota(jnp.int32, (16, W), 1)
    row16 = lax.broadcasted_iota(jnp.int32, (16, W), 0)
    gram_line = jnp.sum(jnp.where(lane16 == row16 + KB, gram_sum, 0.0), axis=0, keepdims=True)
    gram_line = jnp.where(lane16[:1] < IMG, gram_line, 0.0)

    to_right.wait_recv()
    to_left.wait_recv()
    ph = jnp.where(lane < W // 2, halo[0], halo[1])
    halo_part = fold(times(bhalo[...], spread(ph, same)))
    zero1 = jnp.zeros((1, W), F32)
    pre = jnp.concatenate([a + b for a, b in zip(own_part, halo_part)] + [zero1] * 3, axis=0)
    prec[...] = pre

    to_low = pltpu.make_async_remote_copy(
        prec, near.at[1], near_send.at[0], near_recv.at[1], device_id=below, device_id_type=MESH
    )
    to_high = pltpu.make_async_remote_copy(
        prec, near.at[0], near_send.at[1], near_recv.at[0], device_id=above, device_id_type=MESH
    )

    @pl.when(has_low)
    def _():
        to_low.start()

    @pl.when(has_high)
    def _():
        to_high.start()

    rotor_copies = []
    for k in range(3):
        rotor_copies.append(
            pltpu.make_async_remote_copy(
                prec, rotor.at[2 - k], rotor_send.at[k], rotor_recv.at[2 - k],
                device_id=opposite3[k], device_id_type=MESH,
            )
        )

    def cross(k):
        @pl.when(band == 7)
        def _():
            pl.semaphore_wait(met.at[4 + k], 1)

        rotor_copies[k].start()

    @pl.when(at_edge & first)
    def _():
        for k in (1, 2, 0):
            cross(k)

    @pl.when(at_edge & jnp.logical_not(first))
    def _():
        for k in (1, 0, 2):
            cross(k)

    pl.semaphore_wait(met.at[1], len(twos))
    tell(2, [(t0, z, 1 - c, y, xl)])
    column = [moved(here, ("y",), (d,)) for d in (4, 3, 5, 2, 6, 1, 7)]
    tell(3, column)

    edge_right.wait_recv()
    edge_left.wait_recv()
    panel0 = jnp.where(lane < W // 2, ph, own)
    panel1 = jnp.where(lane < W // 2, own, ph)

    def edge_of(side, panel):
        rows = edge_in[side].astype(F32)
        total_row = rows[:, :W] * panel[0:1, :]
        for u in range(1, NC):
            total_row = total_row + rows[:, u * W : (u + 1) * W] * panel[u : u + 1, :]
        return jnp.sum(total_row, axis=1, keepdims=True)

    tm = jnp.where(lane == 0, edge_of(0, panel0), pltpu.roll(pre, 1, 1))
    tp = jnp.where(lane == W - 1, edge_of(1, panel1), pltpu.roll(pre, W - 1, 1))
    base = 6.0 * pre - face[0] * tm - face[1] * tp
    for w in range(NC):
        base = base + jac[w] * pre[w : w + 1, :]
    image_buf[...] = base

    @pl.when(has_low)
    def _():
        to_high.wait_recv()

    @pl.when(has_high)
    def _():
        to_low.wait_recv()

    @pl.when(band == 0)
    def _():
        near[0] = jnp.zeros((8, W), F32)

    @pl.when(band == 15)
    def _():
        near[1] = jnp.zeros((8, W), F32)

    @pl.when(at_edge)
    def _():
        for copy in rotor_copies:
            copy.wait_recv()
        shift = off[0] - 4032
        o = jnp.where(band == 7, shift, W - shift)
        joined = jnp.where(
            lane >= 64 + o, rotor[0], jnp.where(lane < o - 64, rotor[2], rotor[1])
        )
        turn = 64 - o
        turn = jnp.where(turn < 0, turn + W, turn)
        crossed = pltpu.roll(joined, turn, 1)

        @pl.when(band == 8)
        def _():
            near[0] = crossed

        @pl.when(band == 7)
        def _():
            near[1] = crossed


    pl.semaphore_wait(met.at[2], 1)

    image = image_buf[...] - face[2] * near[0] - face[3] * near[1]
    image_buf[...] = image

    late = [jnp.sum(basis[i] * image, axis=0, keepdims=True) for i in range(KB)]
    late.append(jnp.sum(image * image, axis=0, keepdims=True))
    late += [zero1] * 3
    late_sum = jnp.sum(jnp.concatenate(late, axis=0), axis=1, keepdims=True)
    want = jnp.where(row < KB, row, IMG)
    want = jnp.where(row > KB, -1, want)
    line = gram_line + jnp.sum(jnp.where(lane == want, late_sum, 0.0), axis=0, keepdims=True)

    ends = []
    for k, axes in enumerate(PHASES):
        src, slots, ssem, rsem = phase_refs[4 * k : 4 * k + 4]
        some = offsets_of(axes)
        n = len(some)
        src[...] = line
        if k == 1:
            pl.semaphore_wait(met.at[3], len(column))
        for s, o in enumerate(some):
            pltpu.make_async_remote_copy(
                src, slots.at[pl.ds(s, 1), :], ssem, rsem,
                device_id=moved(here, axes, o), device_id_type=MESH,
            ).start()
        everything = slots.at[pl.ds(0, n), :]
        whole = pltpu.make_async_remote_copy(
            everything, everything, ssem, rsem, device_id=right, device_id_type=MESH
        )
        whole.wait_recv()
        ends.append(whole)
        line = line + jnp.sum(slots[pl.ds(0, n), :], axis=0, keepdims=True)

    line_out[...] = line

    for copy in [to_left, to_right, edge_left, edge_right] + ends:
        copy.wait_send()

    @pl.when(has_low)
    def _():
        to_low.wait_send()

    @pl.when(has_high)
    def _():
        to_high.wait_send()

    @pl.when(at_edge)
    def _():
        for copy in rotor_copies:
            copy.wait_send()


def finish(total, image, prec, line_in, basis, precond_out, v_out, hess_out):
    line = line_in[...] * (1.0 / total)
    lane16 = lax.broadcasted_iota(jnp.int32, (16, W), 1)
    row16 = lax.broadcasted_iota(jnp.int32, (16, W), 0)
    spread16 = jnp.sum(jnp.where(lane16 == row16, line, 0.0), axis=1, keepdims=True)
    at = [jnp.broadcast_to(spread16[i : i + 1, :], (1, W)) for i in range(IMG + 1)]
    proj = at[:KB]
    gram = {pair: at[KB + k] for k, pair in enumerate(PAIRS)}
    squares = at[IMG]
    ortho = image[...]
    for i in range(KB):
        squares = squares - 2.0 * proj[i] * proj[i]
        ortho = ortho - proj[i] * basis[i]
    for (a, b), g in gram.items():
        term = proj[a] * g * proj[b]
        squares = squares + (term if a == b else 2.0 * term)
    hnorm = jnp.sqrt(squares + 1e-06)
    v = ortho / hnorm
    for u in range(NC):
        precond_out[u] = prec[u : u + 1, :]
        v_out[u] = v[u : u + 1, :]
    hess_out[...] = jnp.where(lane16[:1] < KB, line, hnorm)[0, : KB + 1]


def on_device(basis, jac_block, face_coef, panel_inverse, rotor_offset):
    total = basis.shape[1] * basis.shape[2] * basis.shape[3] * lax.axis_size(NAMES)
    row = jax.ShapeDtypeStruct((NC, 1, W), F32)
    arrays = (basis, jac_block, face_coef, panel_inverse)
    vmem = pl.BlockSpec(memory_space=pltpu.VMEM)
    dma = pltpu.SemaphoreType.DMA
    phase_shapes = []
    for axes in PHASES:
        n = len(offsets_of(axes))
        phase_shapes += [
            pltpu.VMEM((1, W), F32),
            pltpu.VMEM(((n + 7) // 8 * 8, W), F32),
            dma,
            dma,
        ]
    tile = jax.ShapeDtypeStruct((8, W), F32)
    hbm = pl.BlockSpec(memory_space=pltpu.HBM)
    image, precond, line, basis_tiles = pl.pallas_call(
        functools.partial(kernel, float(total)),
        out_shape=(
            tile,
            tile,
            jax.ShapeDtypeStruct((1, W), F32),
            jax.ShapeDtypeStruct((KB, 8, W), F32),
        ),
        in_specs=[hbm] * 4 + [pl.BlockSpec(memory_space=pltpu.SMEM)],
        out_specs=(vmem,) * 4,
        scratch_shapes=[
            pltpu.VMEM((NC, 8, W), F32),
            pltpu.VMEM((4, 8, W), F32),
            pltpu.VMEM((2, 320, 640), jnp.bfloat16),
            pltpu.VMEM((8, W), F32),
            pltpu.VMEM((2, 8, W), F32),
            pltpu.VMEM((2, 8, 640), jnp.bfloat16),
            pltpu.VMEM((2, 8, 640), jnp.bfloat16),
            pltpu.VMEM((320, 640), jnp.bfloat16),
            pltpu.VMEM((320, 640), jnp.bfloat16),
            pltpu.VMEM((2, 8, W), F32),
            pltpu.VMEM((3, 8, W), F32),
            pltpu.SemaphoreType.REGULAR((7,)),
            dma((14,)),
            dma((2,)),
            dma((2,)),
            dma((2,)),
            dma((2,)),
            dma((2,)),
            dma((2,)),
            dma((3,)),
            dma((3,)),
            *phase_shapes,
        ],
        compiler_params=pltpu.CompilerParams(
            collective_id=0, has_side_effects=True, vmem_limit_bytes=8 << 20
        ),
        name="schwarz_step",
    )(*[pltpu.with_memory_space_constraint(a, pltpu.HBM) for a in arrays], rotor_offset)
    return pl.pallas_call(
        functools.partial(finish, float(total)),
        out_shape=(row, row, jax.ShapeDtypeStruct((KB + 1,), F32)),
        in_specs=[vmem] * 4,
        out_specs=(vmem,) * 3,
        compiler_params=pltpu.CompilerParams(vmem_limit_bytes=4 << 20),
        name="schwarz_finish",
    )(image, precond, line, basis_tiles)


def solution(mesh):
    finer = Mesh(mesh.devices.reshape(4, 8, 2, 8, 2), NAMES)
    in_specs = (
        P(None, None, BAND, THETA),
        P(None, None, BAND, THETA),
        P(None, None, BAND, THETA),
        P(BAND, THETA, None, None),
        P(),
    )
    out_specs = (P(None, BAND, THETA), P(None, BAND, THETA), P())
    return jax.shard_map(
        on_device, mesh=finer, in_specs=in_specs, out_specs=out_specs, check_vma=False
    )
```

```python
import functools
import itertools

import jax
import jax.numpy as jnp
from jax import lax
from jax.experimental import pallas as pl
from jax.experimental.pallas import tpu as pltpu
from jax.sharding import Mesh
from jax.sharding import PartitionSpec as P

THETA = ("theta_0", "theta_1", "theta_2")
BAND = ("band_0", "band_1")
NAMES = ("theta_0", "theta_1", "theta_2", "band_0", "band_1")
MESH = pl.DeviceIdType.MESH

SIZES = {"x": 8, "y": 8, "z": 8, "c": 2}
PHASES = (("z", "c"), ("x", "y"))
F32 = jnp.float32
KB, NC, W = 4, 5, 128
PAIRS = [(a, b) for a in range(KB) for b in range(a, KB)]
IMG = KB + len(PAIRS)


def ring_distance(d, n):
    return min(d, n - d)


def offsets_of(axes):
    every = itertools.product(*[range(SIZES[a]) for a in axes])
    some = [o for o in every if any(o)]
    return sorted(
        some, key=lambda o: -sum(ring_distance(d, SIZES[a]) for d, a in zip(o, axes))
    )


def add_mod(v, d, n):
    if d == 0:
        return v
    s = v + d
    return jnp.where(s >= n, s - n, s)


def moved(here, axes, offset):
    t0, z, c, y, xl = here
    for a, d in zip(axes, offset):
        if d == 0:
            continue
        if a == "x":
            if d % 2:
                s = t0 + xl + d // 2
                t0 = jnp.where(s >= 4, s - 4, s)
                xl = 1 - xl
            else:
                t0 = add_mod(t0, d // 2, 4)
        elif a == "y":
            y = add_mod(y, d, 8)
        elif a == "z":
            z = add_mod(z, d, 8)
        else:
            c = 1 - c
    return (t0, z, c, y, xl)


def theta_next(here):
    t0, z, c, y, xl = here
    z1 = z + c
    over = z1 >= 8
    t1 = jnp.where(over, t0 + 1, t0)
    return (jnp.where(t1 >= 4, t1 - 4, t1), jnp.where(over, 0, z1), 1 - c, y, xl)


def theta_prev(here):
    t0, z, c, y, xl = here
    z1 = z - 1 + c
    under = z1 < 0
    t1 = jnp.where(under, t0 - 1, t0)
    return (jnp.where(t1 < 0, t1 + 4, t1), jnp.where(under, 7, z1), 1 - c, y, xl)


def band_next(here):
    t0, z, c, y, xl = here
    y1 = y + xl
    return (t0, z, c, jnp.where(y1 >= 8, y1 - 8, y1), 1 - xl)


def band_prev(here):
    t0, z, c, y, xl = here
    y1 = y - 1 + xl
    return (t0, z, c, jnp.where(y1 < 0, y1 + 8, y1), 1 - xl)


def across(here):
    t0, z, c, y, xl = here
    return (add_mod(t0, 2, 4), z, c, 7 - y, 1 - xl)


def kernel(
    total,
    basis_hbm,
    jac_hbm,
    face_hbm,
    pinv_hbm,
    off,
    image_buf,
    prec,
    line_out,
    basis,
    jac,
    face,
    pinv,
    halo,
    edge_out,
    edge_in,
    bown,
    bhalo,
    near,
    rotor,
    met,
    load_sems,
    halo_send,
    halo_recv,
    edge_send,
    edge_recv,
    near_send,
    near_recv,
    rotor_send,
    rotor_recv,
    *phase_refs,
):
    here = tuple(lax.axis_index(n) for n in NAMES)
    t0, z, c, y, xl = here
    band = y * 2 + xl
    at_edge = (band == 7) | (band == 8)
    first = (z == 0) & (c == 0)
    has_low = (band != 0) & (band != 8)
    has_high = (band != 7) & (band != 15)
    left, right = theta_prev(here), theta_next(here)
    below, above = band_prev(here), band_next(here)
    opposite = across(here)
    opposite3 = (theta_prev(opposite), opposite, theta_next(opposite))

    loads = []
    zero3 = jnp.zeros((3, W), F32)
    for i in range(KB):
        loads.append((basis_hbm.at[i, :, 0, :], basis.at[i, pl.ds(0, NC), :], 0 if i == KB - 1 else 1))
    for w in range(NC):
        loads.append((jac_hbm.at[:, w, 0, :], jac.at[w, pl.ds(0, NC), :], 1))
    for d in range(4):
        loads.append((face_hbm.at[d, :, 0, :], face.at[d, pl.ds(0, NC), :], 1))
    copies = [
        pltpu.make_async_copy(src, dst, load_sems.at[k]) for k, (src, dst, _) in enumerate(loads)
    ]
    copies[KB - 1].start()
    pinv_copy = pltpu.make_async_copy(pinv_hbm.at[0], pinv, load_sems.at[len(loads)])
    pinv_copy.start()
    for k, copy in enumerate(copies):
        if k != KB - 1:
            copy.start()

    barrier = pltpu.get_barrier_semaphore()
    ones = [(a, o) for a in "xyz" for o in (1, 7)]
    steps = [moved(here, (a,), (o,)) for a, o in ones]
    partners = [left, right, below, above] + steps
    for p in partners:
        pl.semaphore_signal(barrier, inc=1, device_id=p, device_id_type=MESH)

    @pl.when(band == 7)
    def _():
        for p in opposite3:
            pl.semaphore_signal(barrier, inc=1, device_id=p, device_id_type=MESH)

    def tell(k, devices):
        for p in devices:
            pl.semaphore_signal(met.at[k], inc=1, device_id=p, device_id_type=MESH)

    for i in range(KB):
        basis[i, NC:, :] = zero3
    for w in range(NC):
        jac[w, NC:, :] = zero3
    for d in range(4):
        face[d, NC:, :] = zero3

    lane = lax.broadcasted_iota(jnp.int32, (8, W), 1)
    row = lax.broadcasted_iota(jnp.int32, (8, W), 0)

    pl.semaphore_wait(barrier, len(partners) + jnp.where(band == 8, 3, 0))

    @pl.when(band == 8)
    def _():
        for k in (1, 0, 2):
            tell(6 - k, [opposite3[k]])

    tell(0, steps)

    copies[KB - 1].wait()

    to_left = pltpu.make_async_remote_copy(
        basis.at[KB - 1], halo.at[1], halo_send.at[0], halo_recv.at[1], device_id=left, device_id_type=MESH
    )
    to_right = pltpu.make_async_remote_copy(
        basis.at[KB - 1], halo.at[0], halo_send.at[1], halo_recv.at[0], device_id=right, device_id_type=MESH
    )
    edge_left = pltpu.make_async_remote_copy(
        edge_out.at[0], edge_in.at[1], edge_send.at[0], edge_recv.at[1],
        device_id=left, device_id_type=MESH,
    )
    edge_right = pltpu.make_async_remote_copy(
        edge_out.at[1], edge_in.at[0], edge_send.at[1], edge_recv.at[0],
        device_id=right, device_id_type=MESH,
    )
    to_right.start()

    to_left.start()

    own = pltpu.roll(basis[KB - 1].astype(jnp.bfloat16).astype(F32), W // 2, 1)

    pinv_copy.wait()

    def rows_of(side, k):
        some = [pinv[side, u * 64 + k : u * 64 + k + 1, :].astype(F32) for u in range(NC)]
        return jnp.concatenate(some + [jnp.zeros((3, 640), F32)], axis=0).astype(jnp.bfloat16)

    edge_out[0] = rows_of(0, 0)
    edge_out[1] = rows_of(1, 63)
    edge_right.start()

    edge_left.start()

    cols = lax.broadcasted_iota(jnp.int32, (320, 640), 1) % W
    a0, a1 = pinv[0], pinv[1]
    bown[...] = jnp.where(cols < W // 2, a1, a0)
    bhalo[...] = jnp.where(cols < W // 2, a0, a1)
    xrow = lax.broadcasted_iota(jnp.int32, (W, W), 0)
    xlane = lax.broadcasted_iota(jnp.int32, (W, W), 1)
    same = (xrow < W // 2) == (xlane < W // 2)

    def spread(vec, keep):
        parts = [
            jnp.where(keep, jnp.broadcast_to(vec[u : u + 1, :], (W, W)), 0.0).astype(jnp.bfloat16)
            for u in range(NC)
        ]
        return jnp.concatenate(parts, axis=1)

    def times(mat, rhs):
        return lax.dot_general(
            mat, rhs, (((1,), (1,)), ((), ())), preferred_element_type=F32
        )

    r_own = times(bown[...], spread(own, jnp.logical_not(same)))
    pick = lax.broadcasted_iota(jnp.int32, (64, W), 0) == lax.broadcasted_iota(
        jnp.int32, (64, W), 1
    ) % 64

    def fold(r):
        return [
            jnp.sum(jnp.where(pick, r[u * 64 : (u + 1) * 64, :], 0.0), axis=0, keepdims=True)
            for u in range(NC)
        ]

    own_part = fold(r_own)

    pl.semaphore_wait(met.at[0], len(steps))
    twos = [moved(here, (a,), (2 if o == 1 else 6,)) for a, o in ones]
    tell(1, twos)

    for k, copy in enumerate(copies):
        if k != KB - 1:
            copy.wait()

    gram_rows = [jnp.sum(basis[a] * basis[b], axis=0, keepdims=True) for a, b in PAIRS]
    gram_rows += [jnp.zeros((1, W), F32)] * (16 - len(PAIRS))
    gram_sum = jnp.sum(jnp.concatenate(gram_rows, axis=0), axis=1, keepdims=True)
    lane16 = lax.broadcasted_iota(jnp.int32, (16, W), 1)
    row16 = lax.broadcasted_iota(jnp.int32, (16, W), 0)
    gram_line = jnp.sum(jnp.where(lane16 == row16 + KB, gram_sum, 0.0), axis=0, keepdims=True)
    gram_line = jnp.where(lane16[:1] < IMG, gram_line, 0.0)

    to_right.wait_recv()
    to_left.wait_recv()
    ph = jnp.where(lane < W // 2, halo[1], halo[0]).astype(jnp.bfloat16).astype(F32)
    ph = pltpu.roll(ph, W // 2, 1)
    halo_part = fold(times(bhalo[...], spread(ph, same)))
    zero1 = jnp.zeros((1, W), F32)
    pre = jnp.concatenate([a + b for a, b in zip(own_part, halo_part)] + [zero1] * 3, axis=0)
    prec[...] = pre

    to_low = pltpu.make_async_remote_copy(
        prec, near.at[1], near_send.at[0], near_recv.at[1], device_id=below, device_id_type=MESH
    )
    to_high = pltpu.make_async_remote_copy(
        prec, near.at[0], near_send.at[1], near_recv.at[0], device_id=above, device_id_type=MESH
    )

    @pl.when(has_low)
    def _():
        to_low.start()

    @pl.when(has_high)
    def _():
        to_high.start()

    rotor_copies = []
    for k in range(3):
        rotor_copies.append(
            pltpu.make_async_remote_copy(
                prec, rotor.at[2 - k], rotor_send.at[k], rotor_recv.at[2 - k],
                device_id=opposite3[k], device_id_type=MESH,
            )
        )

    def cross(k):
        @pl.when(band == 7)
        def _():
            pl.semaphore_wait(met.at[4 + k], 1)

        rotor_copies[k].start()

    @pl.when(at_edge & first)
    def _():
        for k in (1, 2, 0):
            cross(k)

    @pl.when(at_edge & jnp.logical_not(first))
    def _():
        for k in (1, 0, 2):
            cross(k)

    pl.semaphore_wait(met.at[1], len(twos))
    tell(2, [(t0, z, 1 - c, y, xl)])
    column = [moved(here, ("y",), (d,)) for d in (4, 3, 5, 2, 6, 1, 7)]
    tell(3, column)

    edge_right.wait_recv()
    edge_left.wait_recv()
    panel0 = jnp.where(lane < W // 2, ph, own)
    panel1 = jnp.where(lane < W // 2, own, ph)

    def edge_of(side, panel):
        rows = edge_in[side].astype(F32)
        total_row = rows[:, :W] * panel[0:1, :]
        for u in range(1, NC):
            total_row = total_row + rows[:, u * W : (u + 1) * W] * panel[u : u + 1, :]
        return jnp.sum(total_row, axis=1, keepdims=True)

    tm = jnp.where(lane == 0, edge_of(0, panel0), pltpu.roll(pre, 1, 1))
    tp = jnp.where(lane == W - 1, edge_of(1, panel1), pltpu.roll(pre, W - 1, 1))
    base = 6.0 * pre - face[0] * tm - face[1] * tp
    for w in range(NC):
        base = base + jac[w] * pre[w : w + 1, :]
    image_buf[...] = base

    @pl.when(has_low)
    def _():
        to_high.wait_recv()

    @pl.when(has_high)
    def _():
        to_low.wait_recv()

    @pl.when(band == 0)
    def _():
        near[0] = jnp.zeros((8, W), F32)

    @pl.when(band == 15)
    def _():
        near[1] = jnp.zeros((8, W), F32)

    @pl.when(at_edge)
    def _():
        for copy in rotor_copies:
            copy.wait_recv()
        shift = off[0] - 4032
        o = jnp.where(band == 7, shift, W - shift)
        joined = jnp.where(
            lane >= 64 + o, rotor[0], jnp.where(lane < o - 64, rotor[2], rotor[1])
        )
        turn = 64 - o
        turn = jnp.where(turn < 0, turn + W, turn)
        crossed = pltpu.roll(joined, turn, 1)

        @pl.when(band == 8)
        def _():
            near[0] = crossed

        @pl.when(band == 7)
        def _():
            near[1] = crossed


    pl.semaphore_wait(met.at[2], 1)

    image = image_buf[...] - face[2] * near[0] - face[3] * near[1]
    image_buf[...] = image

    late = [jnp.sum(basis[i] * image, axis=0, keepdims=True) for i in range(KB)]
    late.append(jnp.sum(image * image, axis=0, keepdims=True))
    late += [zero1] * 3
    late_sum = jnp.sum(jnp.concatenate(late, axis=0), axis=1, keepdims=True)
    want = jnp.where(row < KB, row, IMG)
    want = jnp.where(row > KB, -1, want)
    line = gram_line + jnp.sum(jnp.where(lane == want, late_sum, 0.0), axis=0, keepdims=True)

    ends = []
    for k, axes in enumerate(PHASES):
        src, slots, ssem, rsem = phase_refs[4 * k : 4 * k + 4]
        some = offsets_of(axes)
        n = len(some)
        src[...] = line
        if k == 1:
            pl.semaphore_wait(met.at[3], len(column))
        for s, o in enumerate(some):
            pltpu.make_async_remote_copy(
                src, slots.at[pl.ds(s, 1), :], ssem, rsem,
                device_id=moved(here, axes, o), device_id_type=MESH,
            ).start()
        everything = slots.at[pl.ds(0, n), :]
        whole = pltpu.make_async_remote_copy(
            everything, everything, ssem, rsem, device_id=right, device_id_type=MESH
        )
        whole.wait_recv()
        ends.append(whole)
        line = line + jnp.sum(slots[pl.ds(0, n), :], axis=0, keepdims=True)

    line_out[...] = line

    for copy in [to_left, to_right, edge_left, edge_right] + ends:
        copy.wait_send()

    @pl.when(has_low)
    def _():
        to_low.wait_send()

    @pl.when(has_high)
    def _():
        to_high.wait_send()

    @pl.when(at_edge)
    def _():
        for copy in rotor_copies:
            copy.wait_send()


def finish(total, image, prec, line_in, basis, precond_out, v_out, hess_out):
    line = line_in[...] * (1.0 / total)
    lane16 = lax.broadcasted_iota(jnp.int32, (16, W), 1)
    row16 = lax.broadcasted_iota(jnp.int32, (16, W), 0)
    spread16 = jnp.sum(jnp.where(lane16 == row16, line, 0.0), axis=1, keepdims=True)
    at = [jnp.broadcast_to(spread16[i : i + 1, :], (1, W)) for i in range(IMG + 1)]
    proj = at[:KB]
    gram = {pair: at[KB + k] for k, pair in enumerate(PAIRS)}
    squares = at[IMG]
    ortho = image[...]
    for i in range(KB):
        squares = squares - 2.0 * proj[i] * proj[i]
        ortho = ortho - proj[i] * basis[i]
    for (a, b), g in gram.items():
        term = proj[a] * g * proj[b]
        squares = squares + (term if a == b else 2.0 * term)
    hnorm = jnp.sqrt(squares + 1e-06)
    v = ortho / hnorm
    for u in range(NC):
        precond_out[u] = prec[u : u + 1, :]
        v_out[u] = v[u : u + 1, :]
    hess_out[...] = jnp.where(lane16[:1] < KB, line, hnorm)[0, : KB + 1]


def on_device(basis, jac_block, face_coef, panel_inverse, rotor_offset):
    total = basis.shape[1] * basis.shape[2] * basis.shape[3] * lax.axis_size(NAMES)
    row = jax.ShapeDtypeStruct((NC, 1, W), F32)
    arrays = (basis, jac_block, face_coef, panel_inverse)
    vmem = pl.BlockSpec(memory_space=pltpu.VMEM)
    dma = pltpu.SemaphoreType.DMA
    phase_shapes = []
    for axes in PHASES:
        n = len(offsets_of(axes))
        phase_shapes += [
            pltpu.VMEM((1, W), F32),
            pltpu.VMEM(((n + 7) // 8 * 8, W), F32),
            dma,
            dma,
        ]
    tile = jax.ShapeDtypeStruct((8, W), F32)
    hbm = pl.BlockSpec(memory_space=pltpu.HBM)
    image, precond, line, basis_tiles = pl.pallas_call(
        functools.partial(kernel, float(total)),
        out_shape=(
            tile,
            tile,
            jax.ShapeDtypeStruct((1, W), F32),
            jax.ShapeDtypeStruct((KB, 8, W), F32),
        ),
        in_specs=[hbm] * 4 + [pl.BlockSpec(memory_space=pltpu.SMEM)],
        out_specs=(vmem,) * 4,
        scratch_shapes=[
            pltpu.VMEM((NC, 8, W), F32),
            pltpu.VMEM((4, 8, W), F32),
            pltpu.VMEM((2, 320, 640), jnp.bfloat16),
            pltpu.VMEM((2, 8, W), F32),
            pltpu.VMEM((2, 8, 640), jnp.bfloat16),
            pltpu.VMEM((2, 8, 640), jnp.bfloat16),
            pltpu.VMEM((320, 640), jnp.bfloat16),
            pltpu.VMEM((320, 640), jnp.bfloat16),
            pltpu.VMEM((2, 8, W), F32),
            pltpu.VMEM((3, 8, W), F32),
            pltpu.SemaphoreType.REGULAR((7,)),
            dma((14,)),
            dma((2,)),
            dma((2,)),
            dma((2,)),
            dma((2,)),
            dma((2,)),
            dma((2,)),
            dma((3,)),
            dma((3,)),
            *phase_shapes,
        ],
        compiler_params=pltpu.CompilerParams(
            collective_id=0, has_side_effects=True, vmem_limit_bytes=8 << 20
        ),
        name="schwarz_step",
    )(*[pltpu.with_memory_space_constraint(a, pltpu.HBM) for a in arrays], rotor_offset)
    return pl.pallas_call(
        functools.partial(finish, float(total)),
        out_shape=(row, row, jax.ShapeDtypeStruct((KB + 1,), F32)),
        in_specs=[vmem] * 4,
        out_specs=(vmem,) * 3,
        compiler_params=pltpu.CompilerParams(vmem_limit_bytes=4 << 20),
        name="schwarz_finish",
    )(image, precond, line, basis_tiles)


def solution(mesh):
    finer = Mesh(mesh.devices.reshape(4, 8, 2, 8, 2), NAMES)
    in_specs = (
        P(None, None, BAND, THETA),
        P(None, None, BAND, THETA),
        P(None, None, BAND, THETA),
        P(BAND, THETA, None, None),
        P(),
    )
    out_specs = (P(None, BAND, THETA), P(None, BAND, THETA), P())
    return jax.shard_map(
        on_device, mesh=finer, in_specs=in_specs, out_specs=out_specs, check_vma=False
    )
```
